256 devices in a mesh: groups: 2 (over y), ep: 128 (over x, z, core).
Axes of the slice: x: 4, y: 2, z: 16, core: 2. Of those that a mesh axis runs over, the one named last changes fastest.
The devices are a block of a 4x16x16 slice.
Arguments:
- tokens: bfloat16 [32768, 1440], P(('groups', 'ep')), parts along dimension 0, may hold values from -6 to 6
- expert_ids: int32 [32768, 4], P(('groups', 'ep')), parts along dimension 0, may hold values from 0 to 127, as said below
- combine: float32 [32768, 4], P(('groups', 'ep')), parts along dimension 0, may hold values from 0.05 to 1
- gate_weight: bfloat16 [128, 1440, 1440], P('ep'), may hold values from -0.15625 to 0.15625
- up_weight: bfloat16 [128, 1440, 1440], P('ep'), may hold values from -0.15625 to 0.15625
- down_weight: bfloat16 [128, 1440, 1440], P('ep'), may hold values from -0.15625 to 0.15625
Outputs:
- mixture: bfloat16 [32768, 1440], P(('groups', 'ep')), parts along dimension 0
The draws below stay inside these ranges and needn't reach their ends.
There are 2 independent parts, one for each index of `groups`. The reference program is written for one: setup_inputs(seed, part) draws one part's arguments, and reference() takes and returns one part's arrays. A program takes and returns all parts, laid end to end along the dimension named above; an argument that names none is the same for every part. Nothing has to cross between parts.
Inputs may be any that keep to these rules, and one draw needn't show every extreme that they name: `expert_ids`: each row names 4 different experts. In the rows of one device (aligned blocks of 128 rows) no expert is named more than 8 times, and some expert is named exactly 8 times in every block.
All inputs are finite; a program needn't handle non-finite values.
Results may differ from the reference program's by a relative error of at most 0.0058.
Values may be sent and summed in bfloat16 or wider, within the bound.
No kernel may reach another device: no remote copies, remote signals or barrier semaphores. Data moves between devices by JAX's collectives and lax.ppermute only.
A program may use at most 64 MiB of HBM per device.

```python
import math
import jax
import jax.numpy as jnp
from jax import lax

D = 1440
FF = 1440
TOP = 4
TOK_DEV = 128
EXPERTS = 128
TOKENS = 16384
CAP = 8
N_EP = 128


def route_block(key, ranking):
    cells = EXPERTS * CAP
    expert_of_cell = jnp.arange(cells, dtype=jnp.int32) // CAP
    position_in_expert = ranking[expert_of_cell]
    routing_boost = (4 << 20) // (position_in_expert + 1)
    random_jitter = jax.random.randint(jax.random.fold_in(key, 1), (cells,), 0, 1 << 20, dtype=jnp.int32)
    router_logits = routing_boost + random_jitter
    chosen = jnp.argsort(-router_logits, stable=True)[:TOK_DEV * TOP]
    listed = jnp.sort(expert_of_cell[chosen])
    table = listed.reshape(TOP, TOK_DEV).T
    random_reorder = jax.random.permutation(jax.random.fold_in(key, 2), TOK_DEV)
    return table[random_reorder]


def draw_expert_ids(key, part):
    ranking = jax.random.permutation(jax.random.fold_in(key, 7), EXPERTS).astype(jnp.int32)

    def one_block(index):
        return route_block(jax.random.fold_in(key, 100 + index), ranking)
    blocks = jax.vmap(one_block)(jnp.arange(N_EP, dtype=jnp.int32))
    return blocks.reshape(TOKENS, TOP).astype(jnp.int32)


def steps_of(own_key, dims, split, low, top_value):
    def one(axis_at, blocks):
        draws = jax.random.uniform(jax.random.fold_in(jax.random.fold_in(own_key, 6), axis_at), (blocks,), jnp.float32, low / len(split), top_value / len(split))
        return jnp.repeat(jnp.exp(draws), dims[axis_at] // blocks).reshape((-1,) + (1,) * (len(dims) - axis_at - 1))

    level = one(*split[0])
    for cut in split[1:]:
        level = level * one(*cut)
    return level


def bell_draw(key, extent, spread, reach, cuts=(), kind=jnp.bfloat16):
    entries = spread * jax.random.normal(key, extent, jnp.float32)
    if cuts:
        entries = entries * steps_of(key, extent, cuts, -0.22, 0.18)
    return jnp.clip(entries, -reach, reach).astype(kind)


def setup_inputs(seed: int = 0, part: int = 0) -> dict:
    arg_keys = jax.random.split(jax.random.key(seed), 7)
    own_keys = jax.random.split(jax.random.fold_in(arg_keys[6], part), 7)
    tokens = bell_draw(own_keys[0], (TOKENS, D), 1.0, 6.0, ((0, 128),))
    expert_ids = draw_expert_ids(jax.random.fold_in(jax.random.fold_in(arg_keys[6], part), 71), part)
    combine = jnp.clip(jnp.exp(math.log(1.0) - 2.9957323 * jax.random.uniform(own_keys[2], (TOKENS, TOP), jnp.float32) ** steps_of(own_keys[2], (TOKENS, TOP), ((0, 128),), -0.2, 0.2)), 0.05, 1.0)
    gate_weight = bell_draw(arg_keys[3], (EXPERTS, D, FF), D ** -0.5, 0.15625, ((0, 128),))
    up_weight = bell_draw(arg_keys[4], (EXPERTS, D, FF), D ** -0.5, 0.15625, ((0, 128),))
    down_weight = bell_draw(arg_keys[5], (EXPERTS, FF, D), FF ** -0.5, 0.15625, ((0, 128),))
    return dict(tokens=tokens, expert_ids=expert_ids, combine=combine, gate_weight=gate_weight, up_weight=up_weight, down_weight=down_weight)


alpha_gate = 1.702


def run_expert_block(row_block, gate_proj, up_proj, down_proj):
    gate_part = jnp.dot(row_block, gate_proj, preferred_element_type=jnp.float32)
    up_part = jnp.dot(row_block, up_proj, preferred_element_type=jnp.float32)
    hidden = ((up_part + 1.0) * gate_part * jax.nn.sigmoid(alpha_gate * gate_part)).astype(jnp.bfloat16)
    return jnp.dot(hidden, down_proj, preferred_element_type=jnp.float32).astype(jnp.bfloat16)


def reference(tokens, expert_ids, combine, gate_weight, up_weight, down_weight):
    most_rows = N_EP * CAP

    def per_expert(carry, inputs):
        expert, gate_proj, up_proj, down_proj = inputs
        chosen = expert_ids == expert
        weight_row = jnp.sum(jnp.where(chosen, combine, jnp.zeros_like(combine)), axis=1)
        present = jnp.any(chosen, axis=1)
        indices = jnp.nonzero(present, size=most_rows, fill_value=0)[0].astype(jnp.int32)
        valid = jnp.arange(most_rows, dtype=jnp.int32) < jnp.sum(present.astype(jnp.int32))
        outputs = run_expert_block(tokens[indices], gate_proj, up_proj, down_proj)
        factor = jnp.where(valid, weight_row[indices], jnp.zeros_like(weight_row[indices]))
        rescaled_logits = outputs.astype(jnp.float32) * factor[:, None]
        return carry.at[indices].add(rescaled_logits), None

    total = jnp.zeros(tokens.shape, jnp.float32)
    total, unused = lax.scan(per_expert, total, (jnp.arange(EXPERTS, dtype=jnp.int32), gate_weight, up_weight, down_weight))
    return total.astype(jnp.bfloat16)
```

```python
import functools

import jax
import jax.numpy as jnp
from jax import lax
from jax.experimental import pallas as pl
from jax.experimental.pallas import tpu as pltpu
from jax.sharding import Mesh, PartitionSpec as P


ALPHA = 1.702
X_CHIPS = 4
CORES = 2
SLOTS = 8
LANES = 128
CHUNKS = (6, 4, 4, 2)
FF_TILE = 256
KERNEL_VMEM = 6 << 20

f32, bf16 = jnp.float32, jnp.bfloat16


def vmem():
    return pl.BlockSpec(memory_space=pltpu.VMEM)


def pack_kernel(fanout, tok_ref, ids_ref, comb_ref, out_ref):
    width = tok_ref.shape[0]
    out_ref[:width, :] = tok_ref[...]
    weight = comb_ref[...]
    high = weight.astype(bf16).astype(f32)
    lines = [ids_ref[...].astype(f32), high, weight - high]
    lines.append(jnp.zeros((out_ref.shape[0] - width - 3 * fanout, LANES), f32))
    out_ref[width:, :] = jnp.concatenate(lines, axis=0).astype(bf16)


def pack(tokens, ids, combine):
    width, rows = tokens.shape
    tall = width + (3 * ids.shape[0] + 15) // 16 * 16
    return pl.pallas_call(
        functools.partial(pack_kernel, ids.shape[0]),
        out_shape=jax.ShapeDtypeStruct((tall, rows), bf16),
        in_specs=[vmem()] * 3,
        out_specs=vmem(),
        compiler_params=pltpu.CompilerParams(vmem_limit_bytes=KERNEL_VMEM),
        cost_estimate=pl.CostEstimate(flops=1 << 20, bytes_accessed=1 << 20, transcendentals=0),
        name="pack",
    )(tokens, ids, combine)


def select_kernel(width, fanout, x_ref, *refs):
    out_ref, w_ref = refs[-2:]
    ring = lax.axis_size("z")
    half = LANES // 2
    meta = x_ref[width:, :].astype(f32)
    line = lax.broadcasted_iota(jnp.int32, (LANES, LANES), 0)
    col = lax.broadcasted_iota(jnp.int32, (LANES, LANES), 1)
    peer = line % half // SLOTS
    slot = (line % SLOTS).astype(f32)
    expert = ((peer // CORES * ring + lax.axis_index("z")) * CORES + peer % CORES).astype(f32)
    hit = jnp.zeros((LANES, LANES), f32)
    weight = jnp.zeros((LANES, LANES), f32)
    for k in range(fanout):
        match = meta[k : k + 1, :] == expert
        high = meta[fanout + k : fanout + k + 1, :]
        low = meta[2 * fanout + k : 2 * fanout + k + 1, :]
        hit = jnp.where(match, 1.0, hit)
        weight = jnp.where(match, jnp.where(line < half, high, low), weight)
    before = jnp.where(line < col, 1.0, 0.0).astype(bf16)
    rank = jnp.dot(hit.astype(bf16), before, preferred_element_type=f32)
    pick = jnp.where(rank == slot, hit, 0.0)
    w_ref[...] = (pick * weight).astype(bf16)
    chosen = lax.dot_general(
        pick[:half, :].astype(bf16),
        x_ref[:width, :],
        (((1,), (1,)), ((), ())),
        preferred_element_type=f32,
    ).astype(bf16)
    out_ref[...] = chosen.reshape(half // SLOTS, SLOTS, width)


def select(block, buffer, place, count, width, fanout):
    peers = LANES // 2 // SLOTS
    out_shape = (
        jax.ShapeDtypeStruct((peers, count * SLOTS, width), bf16),
        jax.ShapeDtypeStruct((LANES, LANES), bf16),
    )
    operands = (block,) + (() if buffer is None else (buffer,))
    in_specs = [pl.BlockSpec(block.shape, lambda i: (0, 0))]
    if buffer is not None:
        in_specs.append(pl.BlockSpec(memory_space=pl.ANY))
    return pl.pallas_call(
        functools.partial(select_kernel, width, fanout),
        grid=(1,),
        out_shape=out_shape,
        in_specs=in_specs,
        out_specs=(
            pl.BlockSpec((peers, SLOTS, width), lambda i: (0, place, 0)),
            pl.BlockSpec((LANES, LANES), lambda i: (0, 0)),
        ),
        input_output_aliases={} if buffer is None else {1: 0},
        compiler_params=pltpu.CompilerParams(vmem_limit_bytes=KERNEL_VMEM),
        cost_estimate=pl.CostEstimate(flops=1 << 30, bytes_accessed=1 << 20, transcendentals=0),
        name="select",
    )(*operands)


def combine_kernel(w_ref, ret_ref, *refs):
    out_ref = refs[-1]
    width = ret_ref.shape[-1]
    answers = ret_ref[...].reshape(-1, width)
    total = lax.dot_general(
        jnp.concatenate([answers, answers], axis=0),
        w_ref[...],
        (((0,), (0,)), ((), ())),
        preferred_element_type=f32,
    )
    for ref in refs[:-1]:
        total = total + ref[...].astype(f32)
    out_ref[...] = total.astype(bf16)


def combine_step(weights, returned, place, *partials):
    rows = weights.shape[1]
    peers, _, width = returned.shape
    whole = pl.BlockSpec((width, rows), lambda i: (0, 0))
    return pl.pallas_call(
        combine_kernel,
        grid=(1,),
        out_shape=jax.ShapeDtypeStruct((width, rows), bf16),
        in_specs=[
            pl.BlockSpec(weights.shape, lambda i: (0, 0)),
            pl.BlockSpec((peers, SLOTS, width), lambda i: (0, place, 0)),
        ]
        + [whole] * len(partials),
        out_specs=whole,
        compiler_params=pltpu.CompilerParams(vmem_limit_bytes=KERNEL_VMEM),
        cost_estimate=pl.CostEstimate(flops=1 << 30, bytes_accessed=1 << 20, transcendentals=0),
        name="combine",
    )(weights, returned, *partials)


def tiles(width, tile, body):
    whole = width // tile

    @pl.loop(0, whole)
    def _(j):
        body(pl.ds(pl.multiple_of(j * tile, tile), tile))

    if width % tile:
        body(pl.ds(whole * tile, width % tile))


def hidden_kernel(x_ref, gate_ref, up_ref, out_ref):
    rows = x_ref[...]

    def part(cols):
        gate = jnp.dot(rows, gate_ref[:, cols], preferred_element_type=f32)
        up = jnp.dot(rows, up_ref[:, cols], preferred_element_type=f32)
        out_ref[:, cols] = ((up + 1.0) * gate * jax.nn.sigmoid(ALPHA * gate)).astype(bf16)

    tiles(out_ref.shape[1], FF_TILE, part)


def down_kernel(x_ref, down_ref, out_ref):
    rows = x_ref[...]

    def part(cols):
        out_ref[:, cols] = jnp.dot(
            rows, down_ref[:, cols], preferred_element_type=f32
        ).astype(bf16)

    tiles(out_ref.shape[1], FF_TILE, part)


def matmul_call(body, rows, *weights):
    flops = 2 * rows.shape[0] * sum(w.size for w in weights)
    return pl.pallas_call(
        body,
        out_shape=jax.ShapeDtypeStruct((rows.shape[0], weights[0].shape[1]), bf16),
        in_specs=[vmem()] * (1 + len(weights)),
        out_specs=vmem(),
        compiler_params=pltpu.CompilerParams(vmem_limit_bytes=KERNEL_VMEM),
        cost_estimate=pl.CostEstimate(flops=flops, bytes_accessed=1 << 20, transcendentals=0),
    )(rows, *weights)


def arrivals(ring):
    reach = ring // 2
    keys = [("f", 0)]
    for step in range(1, reach + 1):
        keys.append(("f", step))
        if step < reach:
            keys.append(("s", step))
    return keys


def on_device(tokens, expert_ids, combine, gate_weight, up_weight, down_weight):
    ring = lax.axis_size("z")
    width = tokens.shape[1]
    fanout = expert_ids.shape[1]
    weights = (gate_weight[0], up_weight[0], down_weight[0])

    outward = [(z * CORES, (z + 1) % ring * CORES) for z in range(ring)]
    outward += [(z * CORES + 1, (z - 1) % ring * CORES + 1) for z in range(ring)]
    homeward = [(b, a) for a, b in outward]

    def hop(v, pairs):
        return lax.ppermute(v, ("z", "core"), pairs)

    def swap(v):
        return lax.ppermute(v, "core", [(0, 1), (1, 0)])

    def exchange(v):
        return lax.all_to_all(v, ("x", "core"), split_axis=0, concat_axis=0, tiled=True)

    own = pack(tokens.T, expert_ids.T, combine.T)
    blocks = {("f", 0): own}
    blocks["s", 0] = swap(own)
    order = arrivals(ring)
    for stream, step in order[1:]:
        blocks[stream, step] = hop(blocks[stream, step - 1], outward)

    located, mixing, answered = {}, {}, []
    at = 0
    for number, count in enumerate(CHUNKS):
        buffer = None
        for place in range(count):
            key = order[at + place]
            buffer, mixing[key] = select(blocks[key], buffer, place, count, width, fanout)
            located[key] = (number, place)
        at += count
        arrived = exchange(buffer)
        hidden = matmul_call(hidden_kernel, arrived.reshape(-1, width), *weights[:2])
        answers = matmul_call(down_kernel, hidden, weights[2])
        answered.append(exchange(answers.reshape(arrived.shape)))

    def step_of(key, *partials):
        number, place = located[key]
        return combine_step(mixing[key], answered[number], place, *partials)

    sums = {"f": (), "s": ()}
    for stream, step in reversed(order[1:]):
        part = step_of((stream, step), *sums[stream])
        sums[stream] = (hop(part, homeward),)
    crossed = swap(sums["s"][0])
    return step_of(("f", 0), sums["f"][0], crossed).T


def solution(mesh):
    ring = mesh.shape["ep"] // (X_CHIPS * CORES)
    fine = Mesh(
        mesh.devices.reshape(mesh.shape["groups"], X_CHIPS, ring, CORES),
        ("groups", "x", "z", "core"),
    )
    ep = ("x", "z", "core")
    rows = P(("groups",) + ep, None)
    whole = P(ep, None, None)
    return jax.shard_map(
        on_device,
        mesh=fine,
        in_specs=(rows, rows, rows, whole, whole, whole),
        out_specs=rows,
        check_vma=False,
    )
```

```python
import functools

import jax
import jax.numpy as jnp
from jax import lax
from jax.experimental import pallas as pl
from jax.experimental.pallas import tpu as pltpu
from jax.sharding import Mesh, PartitionSpec as P


ALPHA = 1.702
X_CHIPS = 4
CORES = 2
SLOTS = 8
LANES = 128
CHUNKS = (6, 6, 4)
FF_TILE = 256
SELECT_TILE = 384
MIX_TILE = 384
PARTS = 3
KERNEL_VMEM = 6 << 20
EXPERT_VMEM = 58 << 20
TOGETHER = ((0,), (1,), (2,))

f32, bf16 = jnp.float32, jnp.bfloat16


def vmem():
    return pl.BlockSpec(memory_space=pltpu.VMEM)


def tiles(width, tile, body):
    whole = width // tile

    @pl.loop(0, whole)
    def _(j):
        body(pl.ds(pl.multiple_of(j * tile, tile), tile))

    if width % tile:
        body(pl.ds(whole * tile, width % tile))


def pack_kernel(fanout, tok_ref, ids_ref, comb_ref, out_ref, ids, comb, sems):
    width = tok_ref.shape[0]
    rows = pltpu.make_async_copy(tok_ref, out_ref.at[:width, :], sems.at[0])
    small = (
        pltpu.make_async_copy(ids_ref, ids, sems.at[1]),
        pltpu.make_async_copy(comb_ref, comb, sems.at[2]),
    )
    rows.start()
    for copy in small:
        copy.start()
    for copy in small:
        copy.wait()
    weight = comb[...]
    high = weight.astype(bf16).astype(f32)
    lines = [ids[...].astype(f32), high, weight - high]
    lines.append(jnp.zeros((out_ref.shape[0] - width - 3 * fanout, LANES), f32))
    out_ref[width:, :] = jnp.concatenate(lines, axis=0).astype(bf16)
    rows.wait()


def pack(tokens, ids, combine):
    width, rows = tokens.shape
    tall = width + (3 * ids.shape[0] + 15) // 16 * 16
    return pl.pallas_call(
        functools.partial(pack_kernel, ids.shape[0]),
        out_shape=jax.ShapeDtypeStruct((tall, rows), bf16),
        in_specs=[pl.BlockSpec(memory_space=pltpu.HBM)] * 3,
        out_specs=vmem(),
        scratch_shapes=[
            pltpu.VMEM(ids.shape, ids.dtype),
            pltpu.VMEM(combine.shape, combine.dtype),
            pltpu.SemaphoreType.DMA((3,)),
        ],
        compiler_params=pltpu.CompilerParams(vmem_limit_bytes=KERNEL_VMEM),
        cost_estimate=pl.CostEstimate(flops=1 << 20, bytes_accessed=1 << 20, transcendentals=0),
        name="pack",
    )(tokens, ids, combine)


def select_kernel(width, fanout, x_ref, *refs):
    out_ref, w_ref = refs[-2:]
    ring = lax.axis_size("z")
    half = LANES // 2
    meta = x_ref[width:, :].astype(f32)
    line = lax.broadcasted_iota(jnp.int32, (half, LANES), 0)
    peer = line // SLOTS
    slot = (line % SLOTS).astype(f32)
    expert = ((peer // CORES * ring + lax.axis_index("z")) * CORES + peer % CORES).astype(f32)
    hit = jnp.zeros((half, LANES), f32)
    high = jnp.zeros((half, LANES), f32)
    low = jnp.zeros((half, LANES), f32)
    for k in range(fanout):
        match = meta[k : k + 1, :] == expert
        hit = jnp.where(match, 1.0, hit)
        high = jnp.where(match, meta[fanout + k : fanout + k + 1, :], high)
        low = jnp.where(match, meta[2 * fanout + k : 2 * fanout + k + 1, :], low)
    row = lax.broadcasted_iota(jnp.int32, (LANES, LANES), 0)
    col = lax.broadcasted_iota(jnp.int32, (LANES, LANES), 1)
    before = jnp.where(row < col, 1.0, 0.0).astype(bf16)
    rank = jnp.dot(hit.astype(bf16), before, preferred_element_type=f32)
    pick = jnp.where(rank == slot, hit, 0.0)
    w_ref[:half, :] = (pick * high).astype(bf16)
    w_ref[half:, :] = (pick * low).astype(bf16)
    chosen = pick.astype(bf16)

    def part(cols):
        rows = lax.dot_general(
            chosen, x_ref[cols, :], (((1,), (1,)), ((), ())), preferred_element_type=f32
        )
        out_ref[:, :, cols] = rows.astype(bf16).reshape(half // SLOTS, SLOTS, -1)

    tiles(width, SELECT_TILE, part)


def select(block, buffer, place, count, bank, line, lines, width, fanout):
    peers = LANES // 2 // SLOTS
    out_shape = (
        jax.ShapeDtypeStruct((peers, count * SLOTS, width), bf16),
        jax.ShapeDtypeStruct((lines * LANES, LANES), bf16),
    )
    operands, aliases = [block], {}
    for at, held in enumerate((buffer, bank)):
        if held is not None:
            aliases[len(operands)] = at
            operands.append(held)
    return pl.pallas_call(
        functools.partial(select_kernel, width, fanout),
        grid=(1,),
        out_shape=out_shape,
        in_specs=[pl.BlockSpec(block.shape, lambda i: (0, 0))]
        + [pl.BlockSpec(memory_space=pl.ANY)] * len(aliases),
        out_specs=(
            pl.BlockSpec((peers, SLOTS, width), lambda i: (0, place, 0)),
            pl.BlockSpec((LANES, LANES), lambda i: (line, 0)),
        ),
        input_output_aliases=aliases,
        compiler_params=pltpu.CompilerParams(vmem_limit_bytes=KERNEL_VMEM),
        cost_estimate=pl.CostEstimate(flops=1 << 30, bytes_accessed=1 << 20, transcendentals=0),
        name="select",
    )(*operands)


def combine_kernel(w_ref, ret_ref, *refs):
    out_ref = refs[-1]
    width = ret_ref.shape[-1]
    weights = w_ref[...]

    def part(cols):
        answers = ret_ref[:, :, cols].reshape(LANES // 2, -1)
        total = lax.dot_general(
            jnp.concatenate([answers, answers], axis=0),
            weights,
            (((0,), (0,)), ((), ())),
            preferred_element_type=f32,
        )
        for ref in refs[:-1]:
            total = total + ref[cols, :].astype(f32)
        out_ref[cols, :] = total.astype(bf16)

    tiles(width, MIX_TILE, part)


def combine_step(bank, line, returned, place, *partials):
    rows = bank.shape[1]
    peers, _, width = returned.shape
    whole = pl.BlockSpec((width, rows), lambda i: (0, 0))
    return pl.pallas_call(
        combine_kernel,
        grid=(1,),
        out_shape=jax.ShapeDtypeStruct((width, rows), bf16),
        in_specs=[
            pl.BlockSpec((LANES, rows), lambda i: (line, 0)),
            pl.BlockSpec((peers, SLOTS, width), lambda i: (0, place, 0)),
        ]
        + [whole] * len(partials),
        out_specs=whole,
        compiler_params=pltpu.CompilerParams(vmem_limit_bytes=KERNEL_VMEM),
        cost_estimate=pl.CostEstimate(flops=1 << 30, bytes_accessed=1 << 20, transcendentals=0),
        name="combine",
    )(bank, returned, *partials)


def expert_kernel(sets, *refs):
    sources, matrices = refs[:sets], refs[sets : sets + 3]
    results = refs[sets + 3 : 2 * sets + 3]
    held, gate, hidden, w_sems = refs[2 * sets + 3 : 2 * sets + 7]
    width = matrices[0].shape[0]
    part = width // PARTS
    if sets > 1:
        x, out, x_sems, out_sems = refs[2 * sets + 7 :]
        taken = [pltpu.make_async_copy(r, x.at[n], x_sems.at[n]) for n, r in enumerate(sources)]
        given = [pltpu.make_async_copy(out.at[n], r, out_sems.at[n]) for n, r in enumerate(results)]
    else:
        taken = given = ()

    def fetch(which):
        for piece in range(PARTS):
            lines = pl.ds(piece * part, part)
            yield pltpu.make_async_copy(
                matrices[which].at[lines, :], held.at[which, lines, :], w_sems.at[which, piece]
            )

    for copy in (*taken, *fetch(0)):
        copy.start()
    for copy in taken:
        copy.wait()

    def stages(x_ref, out_ref, first):
        def ready(which):
            @pl.when(first)
            def _():
                for copy in fetch(which):
                    copy.wait()
                if which < 2:
                    for copy in fetch(which + 1):
                        copy.start()

        def gates(cols):
            gate[:, cols] = jnp.dot(x_ref[...], held[0, :, cols], preferred_element_type=f32)

        def ups(cols):
            up = jnp.dot(x_ref[...], held[1, :, cols], preferred_element_type=f32)
            g = gate[:, cols]
            hidden[:, cols] = ((up + 1.0) * g * jax.nn.sigmoid(ALPHA * g)).astype(bf16)

        def downs(cols):
            out_ref[:, cols] = jnp.dot(
                hidden[...], held[2, :, cols], preferred_element_type=f32
            ).astype(bf16)

        for which, stage in enumerate((gates, ups, downs)):
            ready(which)
            tiles(width, FF_TILE, stage)

    if sets > 1:

        @pl.loop(0, sets)
        def _(n):
            stages(x.at[n], out.at[n], n == 0)
    else:
        stages(sources[0], results[0], True)
    for copy in given:
        copy.start()
    for copy in given:
        copy.wait()


def run_expert(batches, *weights):
    rows, width = batches[0].shape
    sets = len(batches)
    hbm = pl.BlockSpec(memory_space=pltpu.HBM)
    place = hbm if sets > 1 else vmem()
    scratch = [
        pltpu.VMEM((3, width, width), bf16),
        pltpu.VMEM((rows, width), f32),
        pltpu.VMEM((rows, width), bf16),
        pltpu.SemaphoreType.DMA((3, PARTS)),
    ]
    if sets > 1:
        scratch += [pltpu.VMEM((sets, rows, width), bf16)] * 2
        scratch += [pltpu.SemaphoreType.DMA((sets,))] * 2
    return pl.pallas_call(
        functools.partial(expert_kernel, sets),
        out_shape=tuple(jax.ShapeDtypeStruct(x.shape, bf16) for x in batches),
        in_specs=[place] * sets + [hbm] * 3,
        out_specs=(place,) * sets,
        scratch_shapes=scratch,
        compiler_params=pltpu.CompilerParams(vmem_limit_bytes=EXPERT_VMEM),
        cost_estimate=pl.CostEstimate(
            flops=6 * width * width * rows * sets,
            bytes_accessed=6 * width * width,
            transcendentals=0,
        ),
        name="expert",
    )(*batches, *weights)


def arrivals(ring):
    reach = ring // 2
    keys = [("f", 0)]
    for step in range(1, reach + 1):
        keys.append(("f", step))
        if step < reach:
            keys.append(("s", step))
    return keys


def on_device(tokens, expert_ids, combine, gate_weight, up_weight, down_weight):
    ring = lax.axis_size("z")
    width = tokens.shape[1]
    fanout = expert_ids.shape[1]
    weights = (gate_weight[0], up_weight[0], down_weight[0])

    outward = [(z * CORES, (z + 1) % ring * CORES) for z in range(ring)]
    outward += [(z * CORES + 1, (z - 1) % ring * CORES + 1) for z in range(ring)]
    homeward = [(b, a) for a, b in outward]

    def hop(v, pairs):
        return lax.ppermute(v, ("z", "core"), pairs)

    def swap(v):
        return lax.ppermute(v, "core", [(0, 1), (1, 0)])

    def exchange(v):
        return lax.all_to_all(v, ("x", "core"), split_axis=0, concat_axis=0, tiled=True)

    own = pack(tokens.T, expert_ids.T, combine.T)
    blocks = {("f", 0): own}
    blocks["s", 0] = swap(own)
    order = arrivals(ring)
    for stream, step in order[1:]:
        blocks[stream, step] = hop(blocks[stream, step - 1], outward)

    located, bank, received, answered = {}, None, [], {}
    at = 0
    for number, count in enumerate(CHUNKS):
        buffer = None
        for place in range(count):
            key = order[at + place]
            buffer, bank = select(
                blocks[key], buffer, place, count, bank, at + place, len(order), width, fanout
            )
            located[key] = (at + place, number, place)
        at += count
        arrived = exchange(buffer)
        received.append(arrived)
    for group in TOGETHER:
        answers = run_expert([received[n].reshape(-1, width) for n in group], *weights)
        for number, answer in zip(group, answers):
            answered[number] = exchange(answer.reshape(received[number].shape))

    def step_of(key, *partials):
        line, number, place = located[key]
        return combine_step(bank, line, answered[number], place, *partials)

    sums = {"f": (), "s": ()}
    for stream, step in reversed(order[1:]):
        part = step_of((stream, step), *sums[stream])
        sums[stream] = (hop(part, homeward),)
    crossed = swap(sums["s"][0])
    return step_of(("f", 0), sums["f"][0], crossed).T


def solution(mesh):
    ring = mesh.shape["ep"] // (X_CHIPS * CORES)
    fine = Mesh(
        mesh.devices.reshape(mesh.shape["groups"], X_CHIPS, ring, CORES),
        ("groups", "x", "z", "core"),
    )
    ep = ("x", "z", "core")
    rows = P(("groups",) + ep, None)
    whole = P(ep, None, None)
    return jax.shard_map(
        on_device,
        mesh=fine,
        in_specs=(rows, rows, rows, whole, whole, whole),
        out_specs=rows,
        check_vma=False,
    )
```

```python
import functools

import jax
import jax.numpy as jnp
from jax import lax
from jax.experimental import pallas as pl
from jax.experimental.pallas import tpu as pltpu
from jax.sharding import Mesh, PartitionSpec as P


ALPHA = 1.702
X_CHIPS = 4
CORES = 2
SLOTS = 8
LANES = 128
CHUNKS = (4, 4, 4, 4)
TOGETHER = ((0, 1), (2,), (3,))
FF_TILE = 256
SELECT_TILE = 384
MIX_TILE = 384
PARTS = 2
KERNEL_VMEM = 6 << 20
EXPERT_VMEM = 58 << 20
PACK_VMEM = 67043328

f32, bf16 = jnp.float32, jnp.bfloat16


def vmem():
    return pl.BlockSpec(memory_space=pltpu.VMEM)


def tiles(width, tile, body):
    whole = width // tile

    @pl.loop(0, whole)
    def _(j):
        body(pl.ds(pl.multiple_of(j * tile, tile), tile))

    if width % tile:
        body(pl.ds(whole * tile, width % tile))


def pack_kernel(fanout, tok_ref, ids_ref, comb_ref, out_ref, ids, comb, sems):
    width = tok_ref.shape[0]
    rows = pltpu.make_async_copy(tok_ref, out_ref.at[:width, :], sems.at[0])
    small = (
        pltpu.make_async_copy(ids_ref, ids, sems.at[1]),
        pltpu.make_async_copy(comb_ref, comb, sems.at[2]),
    )
    rows.start()
    for copy in small:
        copy.start()
    for copy in small:
        copy.wait()
    weight = comb[...]
    high = weight.astype(bf16).astype(f32)
    lines = [ids[...].astype(f32), high, weight - high]
    lines.append(jnp.zeros((out_ref.shape[0] - width - 3 * fanout, LANES), f32))
    out_ref[width:, :] = jnp.concatenate(lines, axis=0).astype(bf16)
    rows.wait()


def pack(tokens, ids, combine):
    width, rows = tokens.shape
    tall = width + (3 * ids.shape[0] + 15) // 16 * 16
    return pl.pallas_call(
        functools.partial(pack_kernel, ids.shape[0]),
        out_shape=jax.ShapeDtypeStruct((tall, rows), bf16),
        in_specs=[pl.BlockSpec(memory_space=pltpu.HBM)] * 3,
        out_specs=vmem(),
        scratch_shapes=[
            pltpu.VMEM(ids.shape, ids.dtype),
            pltpu.VMEM(combine.shape, combine.dtype),
            pltpu.SemaphoreType.DMA((3,)),
        ],
        compiler_params=pltpu.CompilerParams(vmem_limit_bytes=PACK_VMEM),
        cost_estimate=pl.CostEstimate(flops=1 << 20, bytes_accessed=1 << 20, transcendentals=0),
        name="pack",
    )(tokens, ids, combine)


def select_kernel(width, fanout, x_ref, *refs):
    out_ref, w_out, w_ref, sem = refs[-4:]
    ring = lax.axis_size("z")
    half = LANES // 2
    meta = x_ref[width:, :].astype(f32)
    line = lax.broadcasted_iota(jnp.int32, (half, LANES), 0)
    peer = line // SLOTS
    slot = (line % SLOTS).astype(f32)
    expert = ((peer // CORES * ring + lax.axis_index("z")) * CORES + peer % CORES).astype(f32)
    hit = jnp.zeros((half, LANES), f32)
    high = jnp.zeros((half, LANES), f32)
    low = jnp.zeros((half, LANES), f32)
    for k in range(fanout):
        match = meta[k : k + 1, :] == expert
        hit = jnp.where(match, 1.0, hit)
        high = jnp.where(match, meta[fanout + k : fanout + k + 1, :], high)
        low = jnp.where(match, meta[2 * fanout + k : 2 * fanout + k + 1, :], low)
    row = lax.broadcasted_iota(jnp.int32, (LANES, LANES), 0)
    col = lax.broadcasted_iota(jnp.int32, (LANES, LANES), 1)
    before = jnp.where(row < col, 1.0, 0.0).astype(bf16)
    rank = jnp.dot(hit.astype(bf16), before, preferred_element_type=f32)
    pick = jnp.where(rank == slot, hit, 0.0)
    w_ref[:half, :] = (pick * high).astype(bf16)
    w_ref[half:, :] = (pick * low).astype(bf16)
    keep = pltpu.make_async_copy(w_ref, w_out, sem)
    keep.start()
    chosen = pick.astype(bf16)

    def part(cols):
        rows = lax.dot_general(
            chosen, x_ref[cols, :], (((1,), (1,)), ((), ())), preferred_element_type=f32
        )
        out_ref[:, :, cols] = rows.astype(bf16).reshape(half // SLOTS, SLOTS, -1)

    tiles(width, SELECT_TILE, part)
    keep.wait()


def select(block, buffer, place, count, width, fanout):
    peers = LANES // 2 // SLOTS
    operands = (block,) if buffer is None else (block, buffer)
    return pl.pallas_call(
        functools.partial(select_kernel, width, fanout),
        grid=(1,),
        out_shape=(
            jax.ShapeDtypeStruct((peers, count * SLOTS, width), bf16),
            jax.ShapeDtypeStruct((LANES, LANES), bf16),
        ),
        in_specs=[
            pl.BlockSpec(block.shape, lambda i: (0, 0)),
            pl.BlockSpec(memory_space=pl.ANY),
        ][: len(operands)],
        out_specs=(
            pl.BlockSpec((peers, SLOTS, width), lambda i: (0, place, 0)),
            pl.BlockSpec(memory_space=pltpu.HBM),
        ),
        scratch_shapes=[pltpu.VMEM((LANES, LANES), bf16), pltpu.SemaphoreType.DMA],
        input_output_aliases={} if buffer is None else {1: 0},
        compiler_params=pltpu.CompilerParams(vmem_limit_bytes=KERNEL_VMEM),
        cost_estimate=pl.CostEstimate(flops=1 << 30, bytes_accessed=1 << 20, transcendentals=0),
        name="select",
    )(*operands)


def combine_kernel(w_ref, ret_ref, *refs):
    out_ref = refs[-1]
    width = ret_ref.shape[-1]
    weights = w_ref[...]

    def part(cols):
        answers = ret_ref[:, :, cols].reshape(LANES // 2, -1)
        total = lax.dot_general(
            jnp.concatenate([answers, answers], axis=0),
            weights,
            (((0,), (0,)), ((), ())),
            preferred_element_type=f32,
        )
        for ref in refs[:-1]:
            total = total + ref[cols, :].astype(f32)
        out_ref[cols, :] = total.astype(bf16)

    tiles(width, MIX_TILE, part)


def combine_step(weights, returned, place, *partials):
    rows = weights.shape[1]
    peers, _, width = returned.shape
    whole = pl.BlockSpec((width, rows), lambda i: (0, 0))
    return pl.pallas_call(
        combine_kernel,
        grid=(1,),
        out_shape=jax.ShapeDtypeStruct((width, rows), bf16),
        in_specs=[
            pl.BlockSpec(weights.shape, lambda i: (0, 0)),
            pl.BlockSpec((peers, SLOTS, width), lambda i: (0, place, 0)),
        ]
        + [whole] * len(partials),
        out_specs=whole,
        compiler_params=pltpu.CompilerParams(vmem_limit_bytes=KERNEL_VMEM),
        cost_estimate=pl.CostEstimate(flops=1 << 30, bytes_accessed=1 << 20, transcendentals=0),
        name="combine",
    )(weights, returned, *partials)


def expert_kernel(sets, *refs):
    sources, matrices = refs[:sets], refs[sets : sets + 3]
    results = refs[sets + 3 : 2 * sets + 3]
    x, held, gate, hidden, out, x_sems, w_sems, out_sems = refs[2 * sets + 3 :]
    width = matrices[0].shape[0]
    part = width // PARTS

    def fetch(which):
        for piece in range(PARTS):
            lines = pl.ds(piece * part, part)
            yield pltpu.make_async_copy(
                matrices[which].at[lines, :], held.at[which, lines, :], w_sems.at[which, piece]
            )

    def ready(which):
        for copy in fetch(which):
            copy.wait()
        if which < 2:
            for copy in fetch(which + 1):
                copy.start()

    def stages(n, wait):
        def gates(cols):
            gate[:, cols] = jnp.dot(x[n], held[0, :, cols], preferred_element_type=f32)

        def ups(cols):
            up = jnp.dot(x[n], held[1, :, cols], preferred_element_type=f32)
            g = gate[:, cols]
            hidden[:, cols] = ((up + 1.0) * g * jax.nn.sigmoid(ALPHA * g)).astype(bf16)

        def downs(cols):
            out[n, :, cols] = jnp.dot(
                hidden[...], held[2, :, cols], preferred_element_type=f32
            ).astype(bf16)

        for which, stage in enumerate((gates, ups, downs)):
            wait(which)
            tiles(width, FF_TILE, stage)

    taken = [pltpu.make_async_copy(r, x.at[n], x_sems.at[n]) for n, r in enumerate(sources)]
    given = [pltpu.make_async_copy(out.at[n], r, out_sems.at[n]) for n, r in enumerate(results)]
    for copy in (*taken, *fetch(0)):
        copy.start()
    for copy in taken:
        copy.wait()
    if sets == 1:
        stages(0, ready)
    else:

        @pl.loop(0, sets)
        def _(n):
            stages(n, lambda which: pl.when(n == 0)(lambda: ready(which)))

    for copy in given:
        copy.start()
    for copy in given:
        copy.wait()


def run_expert(batches, *weights):
    rows, width = batches[0].shape
    sets = len(batches)
    hbm = pl.BlockSpec(memory_space=pltpu.HBM)
    return pl.pallas_call(
        functools.partial(expert_kernel, sets),
        out_shape=tuple(jax.ShapeDtypeStruct(x.shape, bf16) for x in batches),
        in_specs=[hbm] * (sets + 3),
        out_specs=(hbm,) * sets,
        scratch_shapes=[
            pltpu.VMEM((sets, rows, width), bf16),
            pltpu.VMEM((3, width, width), bf16),
            pltpu.VMEM((rows, width), f32),
            pltpu.VMEM((rows, width), bf16),
            pltpu.VMEM((sets, rows, width), bf16),
            pltpu.SemaphoreType.DMA((sets,)),
            pltpu.SemaphoreType.DMA((3, PARTS)),
            pltpu.SemaphoreType.DMA((sets,)),
        ],
        compiler_params=pltpu.CompilerParams(vmem_limit_bytes=EXPERT_VMEM),
        cost_estimate=pl.CostEstimate(
            flops=6 * width * width * rows * sets,
            bytes_accessed=6 * width * width,
            transcendentals=0,
        ),
        name="expert",
    )(*batches, *weights)


def arrivals(ring):
    reach = ring // 2
    keys = [("f", 0)]
    for step in range(1, reach + 1):
        keys.append(("f", step))
        if step < reach:
            keys.append(("s", step))
    return keys


def on_device(tokens, expert_ids, combine, gate_weight, up_weight, down_weight):
    ring = lax.axis_size("z")
    width = tokens.shape[1]
    fanout = expert_ids.shape[1]
    weights = (gate_weight[0], up_weight[0], down_weight[0])

    outward = [(z * CORES, (z + 1) % ring * CORES) for z in range(ring)]
    outward += [(z * CORES + 1, (z - 1) % ring * CORES + 1) for z in range(ring)]
    homeward = [(b, a) for a, b in outward]

    def hop(v, pairs):
        return lax.ppermute(v, ("z", "core"), pairs)

    def swap(v):
        return lax.ppermute(v, "core", [(0, 1), (1, 0)])

    def exchange(v):
        return lax.all_to_all(v, ("x", "core"), split_axis=0, concat_axis=0, tiled=True)

    own = pack(tokens.T, expert_ids.T, combine.T)
    blocks = {("f", 0): own}
    blocks["s", 0] = swap(own)
    order = arrivals(ring)
    for stream, step in order[1:]:
        blocks[stream, step] = hop(blocks[stream, step - 1], outward)

    located, mixing, received, answered = {}, {}, [], {}
    at = 0
    for number, count in enumerate(CHUNKS):
        buffer = None
        for place in range(count):
            key = order[at + place]
            buffer, mixing[key] = select(blocks[key], buffer, place, count, width, fanout)
            located[key] = (number, place)
        at += count
        arrived = exchange(buffer)
        received.append(arrived)
    for group in TOGETHER:
        answers = run_expert([received[n].reshape(-1, width) for n in group], *weights)
        for number, answer in zip(group, answers):
            answered[number] = exchange(answer.reshape(received[number].shape))

    def step_of(key, *partials):
        number, place = located[key]
        return combine_step(mixing[key], answered[number], place, *partials)

    sums = {"f": (), "s": ()}
    for stream, step in reversed(order[1:]):
        part = step_of((stream, step), *sums[stream])
        sums[stream] = (hop(part, homeward),)
    crossed = swap(sums["s"][0])
    return step_of(("f", 0), sums["f"][0], crossed).T


def solution(mesh):
    ring = mesh.shape["ep"] // (X_CHIPS * CORES)
    fine = Mesh(
        mesh.devices.reshape(mesh.shape["groups"], X_CHIPS, ring, CORES),
        ("groups", "x", "z", "core"),
    )
    ep = ("x", "z", "core")
    rows = P(("groups",) + ep, None)
    whole = P(ep, None, None)
    return jax.shard_map(
        on_device,
        mesh=fine,
        in_specs=(rows, rows, rows, whole, whole, whole),
        out_specs=rows,
        check_vma=False,
    )
```

```python
import functools

import jax
import jax.numpy as jnp
from jax import lax
from jax.experimental import pallas as pl
from jax.experimental.pallas import tpu as pltpu
from jax.sharding import Mesh, PartitionSpec as P


ALPHA = 1.702
X_CHIPS = 4
CORES = 2
SLOTS = 8
LANES = 128
CHUNKS = (4, 4, 4, 4)
TOGETHER = ((0, 1), (2,), (3,))
FF_TILE = 256
SELECT_TILE = 384
MIX_TILE = 384
PARTS = 2
KERNEL_VMEM = 6 << 20
EXPERT_VMEM = 58 << 20
PACK_VMEM = 67043328

f32, bf16 = jnp.float32, jnp.bfloat16


def vmem():
    return pl.BlockSpec(memory_space=pltpu.VMEM)


def tiles(width, tile, body):
    whole = width // tile

    @pl.loop(0, whole)
    def _(j):
        body(pl.ds(pl.multiple_of(j * tile, tile), tile))

    if width % tile:
        body(pl.ds(whole * tile, width % tile))


def pack_kernel(fanout, tok_ref, ids_ref, comb_ref, out_ref, ids, comb, sems):
    width = tok_ref.shape[0]
    rows = pltpu.make_async_copy(tok_ref, out_ref.at[:width, :], sems.at[0])
    small = (
        pltpu.make_async_copy(ids_ref, ids, sems.at[1]),
        pltpu.make_async_copy(comb_ref, comb, sems.at[2]),
    )
    rows.start()
    for copy in small:
        copy.start()
    for copy in small:
        copy.wait()
    weight = comb[...]
    high = weight.astype(bf16).astype(f32)
    lines = [ids[...].astype(f32), high, weight - high]
    lines.append(jnp.zeros((out_ref.shape[0] - width - 3 * fanout, LANES), f32))
    out_ref[width:, :] = jnp.concatenate(lines, axis=0).astype(bf16)
    rows.wait()


def pack(tokens, ids, combine):
    width, rows = tokens.shape
    tall = width + (3 * ids.shape[0] + 15) // 16 * 16
    return pl.pallas_call(
        functools.partial(pack_kernel, ids.shape[0]),
        out_shape=jax.ShapeDtypeStruct((tall, rows), bf16),
        in_specs=[pl.BlockSpec(memory_space=pltpu.HBM)] * 3,
        out_specs=vmem(),
        scratch_shapes=[
            pltpu.VMEM(ids.shape, ids.dtype),
            pltpu.VMEM(combine.shape, combine.dtype),
            pltpu.SemaphoreType.DMA((3,)),
        ],
        compiler_params=pltpu.CompilerParams(vmem_limit_bytes=PACK_VMEM),
        cost_estimate=pl.CostEstimate(flops=1 << 20, bytes_accessed=1 << 20, transcendentals=0),
        name="pack",
    )(tokens, ids, combine)


def select_kernel(width, fanout, x_ref, *refs):
    out_ref, w_out, w_ref, sem = refs[-4:]
    ring = lax.axis_size("z")
    half = LANES // 2
    meta = x_ref[width:, :].astype(f32)
    line = lax.broadcasted_iota(jnp.int32, (half, LANES), 0)
    peer = line // SLOTS
    slot = (line % SLOTS).astype(f32)
    expert = ((peer // CORES * ring + lax.axis_index("z")) * CORES + peer % CORES).astype(f32)
    hit = jnp.zeros((half, LANES), f32)
    high = jnp.zeros((half, LANES), f32)
    low = jnp.zeros((half, LANES), f32)
    for k in range(fanout):
        match = meta[k : k + 1, :] == expert
        hit = jnp.where(match, 1.0, hit)
        high = jnp.where(match, meta[fanout + k : fanout + k + 1, :], high)
        low = jnp.where(match, meta[2 * fanout + k : 2 * fanout + k + 1, :], low)
    row = lax.broadcasted_iota(jnp.int32, (LANES, LANES), 0)
    col = lax.broadcasted_iota(jnp.int32, (LANES, LANES), 1)
    before = jnp.where(row < col, 1.0, 0.0).astype(bf16)
    rank = jnp.dot(hit.astype(bf16), before, preferred_element_type=f32)
    pick = jnp.where(rank == slot, hit, 0.0)
    w_ref[:half, :] = (pick * high).astype(bf16)
    w_ref[half:, :] = (pick * low).astype(bf16)
    keep = pltpu.make_async_copy(w_ref, w_out, sem)
    keep.start()
    chosen = pick.astype(bf16)

    def part(cols):
        rows = lax.dot_general(
            chosen, x_ref[cols, :], (((1,), (1,)), ((), ())), preferred_element_type=f32
        )
        out_ref[:, :, cols] = rows.astype(bf16).reshape(half // SLOTS, SLOTS, -1)

    tiles(width, SELECT_TILE, part)
    keep.wait()


def select(block, buffer, place, count, width, fanout):
    peers = LANES // 2 // SLOTS
    operands = (block,) if buffer is None else (block, buffer)
    return pl.pallas_call(
        functools.partial(select_kernel, width, fanout),
        grid=(1,),
        out_shape=(
            jax.ShapeDtypeStruct((peers, count * SLOTS, width), bf16),
            jax.ShapeDtypeStruct((LANES, LANES), bf16),
        ),
        in_specs=[
            pl.BlockSpec(block.shape, lambda i: (0, 0)),
            pl.BlockSpec(memory_space=pl.ANY),
        ][: len(operands)],
        out_specs=(
            pl.BlockSpec((peers, SLOTS, width), lambda i: (0, place, 0)),
            pl.BlockSpec(memory_space=pltpu.HBM),
        ),
        scratch_shapes=[pltpu.VMEM((LANES, LANES), bf16), pltpu.SemaphoreType.DMA],
        input_output_aliases={} if buffer is None else {1: 0},
        compiler_params=pltpu.CompilerParams(vmem_limit_bytes=KERNEL_VMEM),
        cost_estimate=pl.CostEstimate(flops=1 << 30, bytes_accessed=1 << 20, transcendentals=0),
        name="select",
    )(*operands)


def combine_kernel(w_ref, ret_ref, *refs):
    out_ref = refs[-1]
    width = ret_ref.shape[-1]
    weights = w_ref[...]

    def part(cols):
        answers = ret_ref[:, :, cols].reshape(LANES // 2, -1)
        total = lax.dot_general(
            jnp.concatenate([answers, answers], axis=0),
            weights,
            (((0,), (0,)), ((), ())),
            preferred_element_type=f32,
        )
        for ref in refs[:-1]:
            total = total + ref[cols, :].astype(f32)
        out_ref[cols, :] = total.astype(bf16)

    tiles(width, MIX_TILE, part)


def combine_step(weights, returned, place, *partials):
    rows = weights.shape[1]
    peers, _, width = returned.shape
    whole = pl.BlockSpec((width, rows), lambda i: (0, 0))
    return pl.pallas_call(
        combine_kernel,
        grid=(1,),
        out_shape=jax.ShapeDtypeStruct((width, rows), bf16),
        in_specs=[
            pl.BlockSpec(weights.shape, lambda i: (0, 0)),
            pl.BlockSpec((peers, SLOTS, width), lambda i: (0, place, 0)),
        ]
        + [whole] * len(partials),
        out_specs=whole,
        compiler_params=pltpu.CompilerParams(vmem_limit_bytes=KERNEL_VMEM),
        cost_estimate=pl.CostEstimate(flops=1 << 30, bytes_accessed=1 << 20, transcendentals=0),
        name="combine",
    )(weights, returned, *partials)


def expert_kernel(sets, *refs):
    sources, matrices = refs[:sets], refs[sets : sets + 3]
    results = refs[sets + 3 : 2 * sets + 3]
    x, held, gate, hidden, out, x_sems, w_sems, out_sems = refs[2 * sets + 3 :]
    width = matrices[0].shape[0]
    part = width // PARTS

    def fetch(which):
        for piece in range(PARTS):
            lines = pl.ds(piece * part, part)
            yield pltpu.make_async_copy(
                matrices[which].at[lines, :], held.at[which, lines, :], w_sems.at[which, piece]
            )

    def ready(which):
        for copy in fetch(which):
            copy.wait()
        if which < 2:
            for copy in fetch(which + 1):
                copy.start()

    def gates(cols):
        gate[:, cols] = jnp.dot(x[...], held[0, :, cols], preferred_element_type=f32)

    def ups(cols):
        up = jnp.dot(x[...], held[1, :, cols], preferred_element_type=f32)
        g = gate[:, cols]
        hidden[:, cols] = ((up + 1.0) * g * jax.nn.sigmoid(ALPHA * g)).astype(bf16)

    def downs(cols):
        out[:, cols] = jnp.dot(
            hidden[...], held[2, :, cols], preferred_element_type=f32
        ).astype(bf16)

    rows = x.shape[0] // sets
    taken = [
        pltpu.make_async_copy(r, x.at[pl.ds(n * rows, rows), :], x_sems.at[n])
        for n, r in enumerate(sources)
    ]
    given = [
        pltpu.make_async_copy(out.at[pl.ds(n * rows, rows), :], r, out_sems.at[n])
        for n, r in enumerate(results)
    ]
    for copy in (*taken, *fetch(0)):
        copy.start()
    for copy in taken:
        copy.wait()
    for which, stage in enumerate((gates, ups, downs)):
        ready(which)
        tiles(width, FF_TILE, stage)
    for copy in given:
        copy.start()
    for copy in given:
        copy.wait()


def run_expert(batches, *weights):
    rows, width = batches[0].shape
    sets = len(batches)
    hbm = pl.BlockSpec(memory_space=pltpu.HBM)
    return pl.pallas_call(
        functools.partial(expert_kernel, sets),
        out_shape=tuple(jax.ShapeDtypeStruct(x.shape, bf16) for x in batches),
        in_specs=[hbm] * (sets + 3),
        out_specs=(hbm,) * sets,
        scratch_shapes=[
            pltpu.VMEM((sets * rows, width), bf16),
            pltpu.VMEM((3, width, width), bf16),
            pltpu.VMEM((sets * rows, width), f32),
            pltpu.VMEM((sets * rows, width), bf16),
            pltpu.VMEM((sets * rows, width), bf16),
            pltpu.SemaphoreType.DMA((sets,)),
            pltpu.SemaphoreType.DMA((3, PARTS)),
            pltpu.SemaphoreType.DMA((sets,)),
        ],
        compiler_params=pltpu.CompilerParams(vmem_limit_bytes=EXPERT_VMEM),
        cost_estimate=pl.CostEstimate(
            flops=6 * width * width * rows * sets,
            bytes_accessed=6 * width * width,
            transcendentals=0,
        ),
        name="expert",
    )(*batches, *weights)


def arrivals(ring):
    reach = ring // 2
    keys = [("f", 0)]
    for step in range(1, reach + 1):
        keys.append(("f", step))
        if step < reach:
            keys.append(("s", step))
    return keys


def on_device(tokens, expert_ids, combine, gate_weight, up_weight, down_weight):
    ring = lax.axis_size("z")
    width = tokens.shape[1]
    fanout = expert_ids.shape[1]
    weights = (gate_weight[0], up_weight[0], down_weight[0])

    outward = [(z * CORES, (z + 1) % ring * CORES) for z in range(ring)]
    outward += [(z * CORES + 1, (z - 1) % ring * CORES + 1) for z in range(ring)]
    homeward = [(b, a) for a, b in outward]

    def hop(v, pairs):
        return lax.ppermute(v, ("z", "core"), pairs)

    def swap(v):
        return lax.ppermute(v, "core", [(0, 1), (1, 0)])

    def exchange(v):
        return lax.all_to_all(v, ("x", "core"), split_axis=0, concat_axis=0, tiled=True)

    own = pack(tokens.T, expert_ids.T, combine.T)
    blocks = {("f", 0): own}
    blocks["s", 0] = swap(own)
    order = arrivals(ring)
    for stream, step in order[1:]:
        blocks[stream, step] = hop(blocks[stream, step - 1], outward)

    located, mixing, received, answered = {}, {}, [], {}
    at = 0
    for number, count in enumerate(CHUNKS):
        buffer = None
        for place in range(count):
            key = order[at + place]
            buffer, mixing[key] = select(blocks[key], buffer, place, count, width, fanout)
            located[key] = (number, place)
        at += count
        arrived = exchange(buffer)
        received.append(arrived)
    for group in TOGETHER:
        answers = run_expert([received[n].reshape(-1, width) for n in group], *weights)
        for number, answer in zip(group, answers):
            answered[number] = exchange(answer.reshape(received[number].shape))

    def step_of(key, *partials):
        number, place = located[key]
        return combine_step(mixing[key], answered[number], place, *partials)

    sums = {"f": (), "s": ()}
    for stream, step in reversed(order[1:]):
        part = step_of((stream, step), *sums[stream])
        sums[stream] = (hop(part, homeward),)
    crossed = swap(sums["s"][0])
    return step_of(("f", 0), sums["f"][0], crossed).T


def solution(mesh):
    ring = mesh.shape["ep"] // (X_CHIPS * CORES)
    fine = Mesh(
        mesh.devices.reshape(mesh.shape["groups"], X_CHIPS, ring, CORES),
        ("groups", "x", "z", "core"),
    )
    ep = ("x", "z", "core")
    rows = P(("groups",) + ep, None)
    whole = P(ep, None, None)
    return jax.shard_map(
        on_device,
        mesh=fine,
        in_specs=(rows, rows, rows, whole, whole, whole),
        out_specs=rows,
        check_vma=False,
    )
```

```python
import functools

import jax
import jax.numpy as jnp
from jax import lax
from jax.experimental import pallas as pl
from jax.experimental.pallas import tpu as pltpu
from jax.sharding import Mesh, PartitionSpec as P


ALPHA = 1.702
X_CHIPS = 4
CORES = 2
SLOTS = 8
LANES = 128
CHUNKS = (4, 4, 4, 4)
TOGETHER = ((0, 1), (2,), (3,))
FF_TILE = 256
SELECT_TILE = 256
MIX_TILE = 256
PARTS = 1
KERNEL_VMEM = 6 << 20
EXPERT_VMEM = 58 << 20
PACK_VMEM = 67043328

f32, bf16 = jnp.float32, jnp.bfloat16


def vmem():
    return pl.BlockSpec(memory_space=pltpu.VMEM)


def tiles(width, tile, body):
    whole = width // tile

    @pl.loop(0, whole)
    def _(j):
        body(pl.ds(pl.multiple_of(j * tile, tile), tile))

    if width % tile:
        body(pl.ds(whole * tile, width % tile))


def pack_kernel(fanout, tok_ref, ids_ref, comb_ref, out_ref, ids, comb, sems):
    width = tok_ref.shape[0]
    rows = pltpu.make_async_copy(tok_ref, out_ref.at[:width, :], sems.at[0])
    small = (
        pltpu.make_async_copy(ids_ref, ids, sems.at[1]),
        pltpu.make_async_copy(comb_ref, comb, sems.at[2]),
    )
    rows.start()
    for copy in small:
        copy.start()
    for copy in small:
        copy.wait()
    weight = comb[...]
    high = weight.astype(bf16).astype(f32)
    lines = [ids[...].astype(f32), high, weight - high]
    lines.append(jnp.zeros((out_ref.shape[0] - width - 3 * fanout, LANES), f32))
    out_ref[width:, :] = jnp.concatenate(lines, axis=0).astype(bf16)
    rows.wait()


def pack(tokens, ids, combine):
    width, rows = tokens.shape
    tall = width + (3 * ids.shape[0] + 15) // 16 * 16
    return pl.pallas_call(
        functools.partial(pack_kernel, ids.shape[0]),
        out_shape=jax.ShapeDtypeStruct((tall, rows), bf16),
        in_specs=[pl.BlockSpec(memory_space=pltpu.HBM)] * 3,
        out_specs=vmem(),
        scratch_shapes=[
            pltpu.VMEM(ids.shape, ids.dtype),
            pltpu.VMEM(combine.shape, combine.dtype),
            pltpu.SemaphoreType.DMA((3,)),
        ],
        compiler_params=pltpu.CompilerParams(vmem_limit_bytes=PACK_VMEM),
        cost_estimate=pl.CostEstimate(flops=1 << 20, bytes_accessed=1 << 20, transcendentals=0),
        name="pack",
    )(tokens, ids, combine)


def select_kernel(width, fanout, x_ref, *refs):
    out_ref, w_out, w_ref, sem = refs[-4:]
    ring = lax.axis_size("z")
    half = LANES // 2
    meta = x_ref[width:, :].astype(f32)
    line = lax.broadcasted_iota(jnp.int32, (half, LANES), 0)
    peer = line // SLOTS
    slot = (line % SLOTS).astype(f32)
    expert = ((peer // CORES * ring + lax.axis_index("z")) * CORES + peer % CORES).astype(f32)
    hit = jnp.zeros((half, LANES), f32)
    high = jnp.zeros((half, LANES), f32)
    low = jnp.zeros((half, LANES), f32)
    for k in range(fanout):
        match = meta[k : k + 1, :] == expert
        hit = jnp.where(match, 1.0, hit)
        high = jnp.where(match, meta[fanout + k : fanout + k + 1, :], high)
        low = jnp.where(match, meta[2 * fanout + k : 2 * fanout + k + 1, :], low)
    row = lax.broadcasted_iota(jnp.int32, (LANES, LANES), 0)
    col = lax.broadcasted_iota(jnp.int32, (LANES, LANES), 1)
    before = jnp.where(row < col, 1.0, 0.0).astype(bf16)
    rank = jnp.dot(hit.astype(bf16), before, preferred_element_type=f32)
    pick = jnp.where(rank == slot, hit, 0.0)
    w_ref[:half, :] = (pick * high).astype(bf16)
    w_ref[half:, :] = (pick * low).astype(bf16)
    keep = pltpu.make_async_copy(w_ref, w_out, sem)
    keep.start()
    chosen = pick.astype(bf16)

    def part(cols):
        rows = lax.dot_general(
            chosen, x_ref[cols, :], (((1,), (1,)), ((), ())), preferred_element_type=f32
        )
        out_ref[:, :, cols] = rows.astype(bf16).reshape(half // SLOTS, SLOTS, -1)

    tiles(width, SELECT_TILE, part)
    keep.wait()


def select(block, buffer, place, count, width, fanout):
    peers = LANES // 2 // SLOTS
    operands = (block,) if buffer is None else (block, buffer)
    return pl.pallas_call(
        functools.partial(select_kernel, width, fanout),
        grid=(1,),
        out_shape=(
            jax.ShapeDtypeStruct((peers, count * SLOTS, width), bf16),
            jax.ShapeDtypeStruct((LANES, LANES), bf16),
        ),
        in_specs=[
            pl.BlockSpec(block.shape, lambda i: (0, 0)),
            pl.BlockSpec(memory_space=pl.ANY),
        ][: len(operands)],
        out_specs=(
            pl.BlockSpec((peers, SLOTS, width), lambda i: (0, place, 0)),
            pl.BlockSpec(memory_space=pltpu.HBM),
        ),
        scratch_shapes=[pltpu.VMEM((LANES, LANES), bf16), pltpu.SemaphoreType.DMA],
        input_output_aliases={} if buffer is None else {1: 0},
        compiler_params=pltpu.CompilerParams(vmem_limit_bytes=KERNEL_VMEM),
        cost_estimate=pl.CostEstimate(flops=1 << 30, bytes_accessed=1 << 20, transcendentals=0),
        name="select",
    )(*operands)


def combine_kernel(w_ref, ret_ref, *refs):
    out_ref = refs[-1]
    width = ret_ref.shape[-1]
    weights = w_ref[...]

    def part(cols):
        answers = ret_ref[:, :, cols].reshape(LANES // 2, -1)
        total = lax.dot_general(
            jnp.concatenate([answers, answers], axis=0),
            weights,
            (((0,), (0,)), ((), ())),
            preferred_element_type=f32,
        )
        for ref in refs[:-1]:
            total = total + ref[cols, :].astype(f32)
        out_ref[cols, :] = total.astype(bf16)

    tiles(width, MIX_TILE, part)


def combine_step(weights, returned, place, *partials):
    rows = weights.shape[1]
    peers, _, width = returned.shape
    whole = pl.BlockSpec((width, rows), lambda i: (0, 0))
    return pl.pallas_call(
        combine_kernel,
        grid=(1,),
        out_shape=jax.ShapeDtypeStruct((width, rows), bf16),
        in_specs=[
            pl.BlockSpec(weights.shape, lambda i: (0, 0)),
            pl.BlockSpec((peers, SLOTS, width), lambda i: (0, place, 0)),
        ]
        + [whole] * len(partials),
        out_specs=whole,
        compiler_params=pltpu.CompilerParams(vmem_limit_bytes=KERNEL_VMEM),
        cost_estimate=pl.CostEstimate(flops=1 << 30, bytes_accessed=1 << 20, transcendentals=0),
        name="combine",
    )(weights, returned, *partials)


def expert_kernel(sets, *refs):
    sources, matrices = refs[:sets], refs[sets : sets + 3]
    results = refs[sets + 3 : 2 * sets + 3]
    x, held, gate, hidden, out, x_sems, w_sems, out_sems = refs[2 * sets + 3 :]
    width = matrices[0].shape[0]
    part = width // PARTS

    def fetch(which):
        for piece in range(PARTS):
            lines = pl.ds(piece * part, part)
            yield pltpu.make_async_copy(
                matrices[which].at[lines, :], held.at[which, lines, :], w_sems.at[which, piece]
            )

    def ready(which):
        for copy in fetch(which):
            copy.wait()
        if which < 2:
            for copy in fetch(which + 1):
                copy.start()

    def gates(cols):
        gate[:, cols] = jnp.dot(x[...], held[0, :, cols], preferred_element_type=f32)

    def ups(cols):
        up = jnp.dot(x[...], held[1, :, cols], preferred_element_type=f32)
        g = gate[:, cols]
        hidden[:, cols] = ((up + 1.0) * g * jax.nn.sigmoid(ALPHA * g)).astype(bf16)

    def downs(cols):
        out[:, cols] = jnp.dot(
            hidden[...], held[2, :, cols], preferred_element_type=f32
        ).astype(bf16)

    rows = x.shape[0] // sets
    taken = [
        pltpu.make_async_copy(r, x.at[pl.ds(n * rows, rows), :], x_sems.at[n])
        for n, r in enumerate(sources)
    ]
    given = [
        pltpu.make_async_copy(out.at[pl.ds(n * rows, rows), :], r, out_sems.at[n])
        for n, r in enumerate(results)
    ]
    for copy in (*taken, *fetch(0)):
        copy.start()
    for copy in taken:
        copy.wait()
    for which, stage in enumerate((gates, ups, downs)):
        ready(which)
        tiles(width, FF_TILE, stage)
    for copy in given:
        copy.start()
    for copy in given:
        copy.wait()


def run_expert(batches, *weights):
    rows, width = batches[0].shape
    sets = len(batches)
    hbm = pl.BlockSpec(memory_space=pltpu.HBM)
    return pl.pallas_call(
        functools.partial(expert_kernel, sets),
        out_shape=tuple(jax.ShapeDtypeStruct(x.shape, bf16) for x in batches),
        in_specs=[hbm] * (sets + 3),
        out_specs=(hbm,) * sets,
        scratch_shapes=[
            pltpu.VMEM((sets * rows, width), bf16),
            pltpu.VMEM((3, width, width), bf16),
            pltpu.VMEM((sets * rows, width), f32),
            pltpu.VMEM((sets * rows, width), bf16),
            pltpu.VMEM((sets * rows, width), bf16),
            pltpu.SemaphoreType.DMA((sets,)),
            pltpu.SemaphoreType.DMA((3, PARTS)),
            pltpu.SemaphoreType.DMA((sets,)),
        ],
        compiler_params=pltpu.CompilerParams(vmem_limit_bytes=EXPERT_VMEM),
        cost_estimate=pl.CostEstimate(
            flops=6 * width * width * rows * sets,
            bytes_accessed=6 * width * width,
            transcendentals=0,
        ),
        name="expert",
    )(*batches, *weights)


def arrivals(ring):
    reach = ring // 2
    keys = [("f", 0)]
    for step in range(1, reach + 1):
        keys.append(("f", step))
        if step < reach:
            keys.append(("s", step))
    return keys


def on_device(tokens, expert_ids, combine, gate_weight, up_weight, down_weight):
    ring = lax.axis_size("z")
    width = tokens.shape[1]
    fanout = expert_ids.shape[1]
    weights = (gate_weight[0], up_weight[0], down_weight[0])

    outward = [(z * CORES, (z + 1) % ring * CORES) for z in range(ring)]
    outward += [(z * CORES + 1, (z - 1) % ring * CORES + 1) for z in range(ring)]
    homeward = [(b, a) for a, b in outward]

    def hop(v, pairs):
        return lax.ppermute(v, ("z", "core"), pairs)

    def swap(v):
        return lax.ppermute(v, "core", [(0, 1), (1, 0)])

    def exchange(v):
        return lax.all_to_all(v, ("x", "core"), split_axis=0, concat_axis=0, tiled=True)

    own = pack(tokens.T, expert_ids.T, combine.T)
    blocks = {("f", 0): own}
    blocks["s", 0] = swap(own)
    order = arrivals(ring)
    for stream, step in order[1:]:
        blocks[stream, step] = hop(blocks[stream, step - 1], outward)

    located, mixing, received, answered = {}, {}, [], {}
    at = 0
    for number, count in enumerate(CHUNKS):
        buffer = None
        for place in range(count):
            key = order[at + place]
            buffer, mixing[key] = select(blocks[key], buffer, place, count, width, fanout)
            located[key] = (number, place)
        at += count
        arrived = exchange(buffer)
        received.append(arrived)
    for group in TOGETHER:
        answers = run_expert([received[n].reshape(-1, width) for n in group], *weights)
        for number, answer in zip(group, answers):
            answered[number] = exchange(answer.reshape(received[number].shape))

    def step_of(key, *partials):
        number, place = located[key]
        return combine_step(mixing[key], answered[number], place, *partials)

    sums = {"f": (), "s": ()}
    for stream, step in reversed(order[1:]):
        part = step_of((stream, step), *sums[stream])
        sums[stream] = (hop(part, homeward),)
    crossed = swap(sums["s"][0])
    return step_of(("f", 0), sums["f"][0], crossed).T


def solution(mesh):
    ring = mesh.shape["ep"] // (X_CHIPS * CORES)
    fine = Mesh(
        mesh.devices.reshape(mesh.shape["groups"], X_CHIPS, ring, CORES),
        ("groups", "x", "z", "core"),
    )
    ep = ("x", "z", "core")
    rows = P(("groups",) + ep, None)
    whole = P(ep, None, None)
    return jax.shard_map(
        on_device,
        mesh=fine,
        in_specs=(rows, rows, rows, whole, whole, whole),
        out_specs=rows,
        check_vma=False,
    )
```
